32 devices in a mesh: group: 4 (over y, x), dom: 8 (over z, core).
Axes of the slice: x: 2, y: 2, z: 4, core: 2. Of those that a mesh axis runs over, the one named last changes fastest.
Arguments:
- p_start: float32 [1024, 128], P(('group', 'dom')), may hold values from -60 to 60
- r_start: float32 [1024, 128], P(('group', 'dom')), may hold values from -60 to 60
- diag_shift: float32 [1024, 128], P(('group', 'dom')), may hold values from 0.5 to 2
- shifts: float32 [8], replicated, may hold values from 0.5 to 1.5
- block_values: float32 [1024, 6, 128, 128], P(('group', 'dom')), may hold values from -0.21875 to 0.21875
- block_cols: int32 [1024, 6], P(('group', 'dom')), may hold values from 0 to 95, as said below
- live_slots: int32 [1024], P(('group', 'dom')), may hold values from 2 to 6, as said below
- needed: int32 [32, 4, 16], P(('group', 'dom')), may hold values from 0 to 31
Outputs:
- basis: float32 [17, 1024, 128], P(None, ('group', 'dom'))
- gram: float32 [17, 17], replicated
The draws below stay inside these ranges and needn't reach their ends.
Inputs may be any that keep to these rules, and one draw needn't show every extreme that they name: `block_cols`: slot 0 of block row b is the row itself (b mod 32); a value below 32 names a block row of the same device, a value 32 + k * 16 + h names entry h of the device's list k of needed. Devices with dom index 0 never use list 0 in used slots, devices with the last dom index never list 1. Slots from live_slots on hold values in range but are not used. `live_slots`: the first block row of every device uses all 6 slots. needed[d, k] lists the local block rows that device d reads from its source s_k(d), in the order of its extended field.
All inputs are finite; a program needn't handle non-finite values.
Results may differ from the reference program's by a relative error of at most 0.0001.
Values sent between devices are 32-bit elements; how exact they have to be, the bound alone decides.
No kernel may reach another device: no remote copies, remote signals or barrier semaphores. Data moves between devices by JAX's collectives and lax.ppermute only.
A program may use at most 64 MiB of HBM per device.

```python
import math
import jax
import jax.numpy as jnp
from jax import lax

BS = 128
S = 8
NB = 6
BR_DEV = 32
HALO = 16
NBLK = 1024
N_GROUP = 4
N_DOM = 8


def rough_vector(key):
    total = BR_DEV * N_GROUP * N_DOM
    owners = (jnp.arange(total) // BR_DEV).astype(jnp.float32)
    rise = jnp.exp(math.log(3.0) * owners / max(N_GROUP * N_DOM - 1, 1))
    cell = jnp.exp(jax.random.uniform(jax.random.fold_in(key, 1), (total, BS), jnp.float32, 0.0, math.log(10.0)))
    base = jax.random.normal(jax.random.fold_in(key, 2), (total, BS), jnp.float32)
    return base * cell * rise[:, None] * 0.25


def draw_p_start(key, part):
    return rough_vector(jax.random.fold_in(key, 101))


def draw_r_start(key, part):
    return rough_vector(jax.random.fold_in(key, 202))


def block_pattern(key):
    base_key = jax.random.fold_in(key, 303)
    total = BR_DEV * N_GROUP * N_DOM
    block_ids = jnp.arange(total, dtype=jnp.int32)
    dom_ids = block_ids // BR_DEV % N_DOM
    live = jax.random.randint(jax.random.fold_in(base_key, 1), (total,), 2, NB + 1)
    live = jnp.where(block_ids % BR_DEV == 0, NB, live).astype(jnp.int32)
    local_pick = jax.random.randint(jax.random.fold_in(base_key, 2), (total, NB), 0, BR_DEV)
    source_pick = jax.random.randint(jax.random.fold_in(base_key, 3), (total, NB), 0, 4)
    entry_pick = jax.random.randint(jax.random.fold_in(base_key, 4), (total, NB), 0, HALO)
    remote_pick = jax.random.randint(jax.random.fold_in(base_key, 5), (total, NB), 0, 2)
    missing = (source_pick == 0) & (dom_ids[:, None] == 0) | (source_pick == 1) & (dom_ids[:, None] == N_DOM - 1)
    remote = (remote_pick == 1) & jnp.logical_not(missing)
    cols = jnp.where(remote, BR_DEV + source_pick * HALO + entry_pick, local_pick)
    cols = cols.at[:, 0].set(block_ids % BR_DEV)
    return (cols.astype(jnp.int32), live)


def draw_block_cols(key, part):
    return block_pattern(key)[0]


def draw_live_slots(key, part):
    return block_pattern(key)[1]


def place_ends(values, stream_key, smallest, largest):
    longest = values.shape.index(max(values.shape))
    spots = []
    for shift in (0, 1):
        where = [jax.random.randint(jax.random.fold_in(stream_key, axis), (), 0, length) for axis, length in enumerate(values.shape)]
        where[longest] = (where[longest] + shift) % values.shape[longest]
        spots.append(tuple(where))
    return values.at[spots[0]].set(smallest).at[spots[1]].set(largest)


def shard_levels(own_key, extent, cuts, smallest, largest):
    def one(dim, parts):
        steps = jax.random.uniform(jax.random.fold_in(jax.random.fold_in(own_key, 6), dim), (parts,), jnp.float32, smallest / len(cuts), largest / len(cuts))
        return jnp.repeat(jnp.exp(steps), extent[dim] // parts).reshape((-1,) + (1,) * (len(extent) - dim - 1))

    level = one(*cuts[0])
    for cut in cuts[1:]:
        level = level * one(*cut)
    return level


def bell_draw(rng, shape, width, most, cuts=(), kind=jnp.bfloat16):
    array = jax.random.normal(rng, shape, jnp.float32) * width
    if len(cuts) > 0:
        array = shard_levels(rng, shape, cuts, -0.22, 0.18) * array
    return jnp.clip(array, min=-most, max=most).astype(kind)


def setup_inputs(seed: int = 0) -> dict:
    arg_keys = jax.random.split(jax.random.key(seed), 9)
    p_start = draw_p_start(jax.random.fold_in(arg_keys[8], 71), 0)
    r_start = draw_r_start(jax.random.fold_in(arg_keys[8], 71), 0)
    diag_shift = jnp.clip(jnp.exp(math.log(2.0) - 1.3862944 * jax.random.uniform(arg_keys[2], (NBLK, BS), jnp.float32) ** shard_levels(arg_keys[2], (NBLK, BS), ((0, 32),), -0.2, 0.2)), 0.5, 2.0)
    shifts = jnp.clip(jax.random.uniform(arg_keys[3], (S,), jnp.float32, 0.5, 1.5), 0.5, 1.5)
    block_values = bell_draw(arg_keys[4], (NBLK, NB, BS, BS), (NB * BS) ** -0.5, 0.21875, ((0, 32),), jnp.float32)
    block_cols = draw_block_cols(jax.random.fold_in(arg_keys[8], 71), 0)
    live_slots = draw_live_slots(jax.random.fold_in(arg_keys[8], 71), 0)
    needed = place_ends(jax.random.randint(arg_keys[7], (N_GROUP * N_DOM, 4, HALO), 0, BR_DEV), jax.random.fold_in(arg_keys[7], 1), 0, BR_DEV - 1).astype(jnp.int32)
    return dict(p_start=p_start, r_start=r_start, diag_shift=diag_shift, shifts=shifts, block_values=block_values, block_cols=block_cols, live_slots=live_slots, needed=needed)


def reference(p_start, r_start, diag_shift, shifts, block_values, block_cols, live_slots, needed):
    ndev = N_GROUP * N_DOM
    device_ids = jnp.arange(ndev, dtype=jnp.int32)
    group_ids = device_ids // N_DOM
    dom_ids = device_ids % N_DOM
    sources = [
        group_ids * N_DOM + jnp.maximum(dom_ids - 1, 0),
        group_ids * N_DOM + jnp.minimum(dom_ids + 1, N_DOM - 1),
        ((group_ids - 1) % N_GROUP) * N_DOM + dom_ids,
        ((group_ids + 1) % N_GROUP) * N_DOM + dom_ids,
    ]
    valid = [
        (dom_ids > 0).astype(jnp.float32),
        (dom_ids < N_DOM - 1).astype(jnp.float32),
        jnp.ones((ndev,), jnp.float32),
        jnp.ones((ndev,), jnp.float32),
    ]
    values = block_values.reshape(ndev, BR_DEV, NB, BS, BS)
    columns = block_cols.reshape(ndev, BR_DEV, NB)
    slot_ids = lax.broadcasted_iota(jnp.int32, (NBLK, NB), 1)
    masks = (slot_ids < live_slots[:, None]).astype(jnp.float32).reshape(ndev, BR_DEV, NB)

    def multiply(vector):
        blocks = vector.reshape(ndev, BR_DEV, BS)
        pieces = [blocks]
        for k in range(4):
            pieces.append(blocks[sources[k][:, None], needed[:, k, :]] * valid[k][:, None, None])
        extended = jnp.concatenate(pieces, axis=1)

        def single(item):
            vals, cols, live, ext = item
            picked = ext[cols] * live[:, :, None]
            return jnp.einsum("bsij,bsj->bi", vals, picked, precision=lax.Precision.HIGHEST)

        return lax.map(single, (values, columns, masks, extended)).reshape(NBLK, BS)

    def advance(vector, theta):
        return multiply(vector) + (diag_shift - theta) * vector

    p_fields = [p_start]
    for step in range(1, S + 1):
        p_fields.append(advance(p_fields[-1], shifts[step - 1]))
    r_fields = [r_start]
    for step in range(1, S):
        r_fields.append(advance(r_fields[-1], shifts[step - 1]))
    basis = jnp.stack(p_fields + r_fields)
    gram = jnp.einsum("kbi,lbi->kl", basis, basis, precision=lax.Precision.HIGHEST) / (NBLK * BS)
    return basis, gram
```

```python
import functools
import jax
import jax.numpy as jnp
from jax import lax
from jax.experimental import pallas as pl
from jax.experimental.pallas import tpu as pltpu
from jax.sharding import PartitionSpec as P

ENTRY = 4096
STRIDE = 16


def sweep(a_ref, tbl, ext, halves, rows, nslots, count_at, first_at, before_row=None):
    bs = ext.shape[1]
    half = bs // 2
    low = lax.broadcasted_iota(jnp.int32, (bs, bs), 1) < half

    def row(b, carry):
        if before_row is not None:
            before_row(b)
        base = b * STRIDE

        def pair(k, acc):
            ap, ar = acc
            for u in range(2):
                e = tbl[base + first_at + 2 * k + u]
                slot = lax.shift_right_logical(e, 12)
                c = lax.bitwise_and(e, ENTRY - 1)
                a = a_ref[b * nslots + slot]
                ap = ap + a * ext[pl.ds(c, 1), :]
                ar = ar + a * ext[pl.ds(c + rows, 1), :]
            return ap, ar

        zero = jnp.zeros((bs, bs), jnp.float32)
        ap, ar = lax.fori_loop(0, tbl[base + count_at], pair, (zero, zero))
        both = jnp.where(low, ap + pltpu.roll(ap, half, 1), ar + pltpu.roll(ar, half, 1))
        hi = both.astype(jnp.bfloat16)
        lo = (both - hi.astype(jnp.float32)).astype(jnp.bfloat16)
        at = pl.ds(pl.multiple_of(b * bs, bs), bs)
        halves[at, 0:bs] = hi
        halves[at, bs:] = lo
        return carry

    lax.fori_loop(0, rows, row, 0)


def lane_sums(halves, y, rows, bs):
    half = bs // 2
    r = lax.broadcasted_iota(jnp.int32, (8, 2 * bs), 0)
    c = lax.broadcasted_iota(jnp.int32, (8, 2 * bs), 1) % bs
    pick = (((r == 0) & (c < half)) | ((r == 1) & (c >= half))).astype(jnp.float32).astype(jnp.bfloat16)
    for b in range(0, rows, 2):
        tile = halves[b * bs : (b + 2) * bs, :]
        out = lax.dot_general(pick, tile, (((1,), (1,)), ((), ())), preferred_element_type=jnp.float32)
        for u in range(2):
            y[b + u : b + u + 1, :] = out[0:1, u * bs : (u + 1) * bs]
            y[rows + b + u : rows + b + u + 1, :] = out[1:2, u * bs : (u + 1) * bs]


def diag_term(cur, diag, shifts, step, rows):
    d = diag[...] - shifts[step]
    return jnp.concatenate([d * cur[0:rows, :], d * cur[rows : 2 * rows, :]], axis=0)


def first_kernel(cols, live, need, shifts, cur, diag, a_hbm, out, a_vmem, tbl, ext, halves, y, sems, *, rows, nslots, halo):
    bs = ext.shape[1]

    def copy(b):
        at = pl.ds(b * nslots, nslots)
        return pltpu.make_async_copy(a_hbm.at[at], a_vmem.at[at], sems.at[b])

    def start(b, carry):
        copy(b).start()
        return carry

    lax.fori_loop(0, rows, start, 0)
    far = 10 * rows
    ext[0 : 2 * rows, :] = cur[...]
    ext[far:, :] = jnp.zeros((ext.shape[0] - far, bs), jnp.float32)

    def build(b, carry):
        base = b * STRIDE
        for k in range(2 * nslots):
            tbl[base + 2 + k] = far
        n = live[b]
        nl = jnp.int32(0)
        nr = jnp.int32(0)
        for s in range(nslots):
            used = s < n
            c = cols[b, s]
            local = c < rows
            q = jnp.maximum(c - rows, 0)
            k = q // halo
            row = jnp.where(local, c, 2 * rows * (k + 1) + need[k, q % halo])
            at = jnp.where(used, jnp.where(local, 2 + nl, 2 + nslots + nr), STRIDE - 1)
            tbl[base + at] = s * ENTRY + row
            nl = nl + jnp.where(used & local, 1, 0)
            nr = nr + jnp.where(used & jnp.logical_not(local), 1, 0)
        tbl[base] = (nl + 1) // 2
        tbl[base + 1] = (nr + 1) // 2
        return carry

    lax.fori_loop(0, rows, build, 0)
    sweep(a_vmem, tbl, ext, halves, rows, nslots, 0, 2, lambda b: copy(b).wait())
    lane_sums(halves, y, rows, bs)
    out[...] = y[...] + diag_term(cur, diag, shifts, 0, rows)


def local_kernel(tbl, shifts, cur, diag, a_vmem, out, ext, halves, y, *, step, rows, nslots):
    bs = ext.shape[1]
    far = 10 * rows
    ext[0 : 2 * rows, :] = cur[...]
    ext[far:, :] = jnp.zeros((ext.shape[0] - far, bs), jnp.float32)
    sweep(a_vmem, tbl, ext, halves, rows, nslots, 0, 2)
    lane_sums(halves, y, rows, bs)
    out[...] = y[...] + diag_term(cur, diag, shifts, step, rows)


def remote_kernel(tbl, part, h0, h1, h2, h3, a_vmem, out, ext, halves, y, *, rows, nslots):
    bs = ext.shape[1]
    far = 10 * rows
    for k, h in enumerate((h0, h1, h2, h3)):
        ext[2 * rows * (k + 1) : 2 * rows * (k + 2), :] = h[...]
    ext[far:, :] = jnp.zeros((ext.shape[0] - far, bs), jnp.float32)
    sweep(a_vmem, tbl, ext, halves, rows, nslots, 1, 2 + nslots)
    lane_sums(halves, y, rows, bs)
    out[...] = y[...] + part[...]


def per_device(p_start, r_start, diag_shift, shifts, block_values, block_cols, live_slots, needed):
    rows, bs = p_start.shape
    nslots = block_values.shape[1]
    halo = needed.shape[2]
    depth = shifts.shape[0]
    f32 = jnp.float32
    smem = pl.BlockSpec(memory_space=pltpu.SMEM)
    vmem = pl.BlockSpec(memory_space=pltpu.VMEM)
    anym = pl.BlockSpec(memory_space=pl.ANY)
    field = jax.ShapeDtypeStruct((2 * rows, bs), f32)
    scratch = [
        pltpu.VMEM((11 * rows + 8, bs), f32),
        pltpu.VMEM((rows * bs, 2 * bs), jnp.bfloat16),
        pltpu.VMEM((2 * rows, bs), f32),
    ]
    params = pltpu.CompilerParams(vmem_limit_bytes=24 * 1024 * 1024)
    kw = dict(rows=rows, nslots=nslots)
    a_flat = block_values.reshape(rows * nslots, bs, bs)

    def halos(cur):
        nd, ng = lax.axis_size("dom"), lax.axis_size("group")
        up = [(i, i + 1) for i in range(nd - 1)]
        down = [(i + 1, i) for i in range(nd - 1)]
        gup = [(i, (i + 1) % ng) for i in range(ng)]
        gdown = [((i + 1) % ng, i) for i in range(ng)]
        return (
            lax.ppermute(cur, "dom", up),
            lax.ppermute(cur, "dom", down),
            lax.ppermute(cur, "group", gup),
            lax.ppermute(cur, "group", gdown),
        )

    cur = jnp.concatenate([p_start, r_start], axis=0)
    fields = [cur]
    for step in range(depth):
        h = halos(cur)
        if step == 0:
            part, a_vmem, tbl = pl.pallas_call(
                functools.partial(first_kernel, halo=halo, **kw),
                out_shape=(
                    field,
                    pltpu.VMEM((rows * nslots, bs, bs), f32),
                    jax.ShapeDtypeStruct((rows * STRIDE,), jnp.int32),
                ),
                in_specs=[smem, smem, smem, smem, vmem, vmem, anym],
                out_specs=(vmem, vmem, smem),
                scratch_shapes=scratch + [pltpu.SemaphoreType.DMA((rows,))],
                compiler_params=params,
                name="first",
            )(block_cols, live_slots, needed[0], shifts, cur, diag_shift, a_flat)
        else:
            part = pl.pallas_call(
                functools.partial(local_kernel, step=step, **kw),
                out_shape=field,
                in_specs=[smem, smem, vmem, vmem, vmem],
                out_specs=vmem,
                scratch_shapes=scratch,
                compiler_params=params,
                name="local",
            )(tbl, shifts, cur, diag_shift, a_vmem)
        cur = pl.pallas_call(
            functools.partial(remote_kernel, **kw),
            out_shape=field,
            in_specs=[smem] + [vmem] * 6,
            out_specs=vmem,
            scratch_shapes=scratch,
            compiler_params=params,
            name="remote",
        )(tbl, part, *h, a_vmem)
        fields.append(cur)
    both = jnp.stack(fields).reshape(depth + 1, 2, rows, bs)
    basis = jnp.concatenate([both[:, 0], both[:depth, 1]], axis=0)
    total_cells = rows * bs * lax.axis_size("group") * lax.axis_size("dom")
    local_gram = jnp.einsum("kbi,lbi->kl", basis, basis, precision=lax.Precision.HIGHEST)
    return basis, lax.psum(local_gram, ("group", "dom")) / total_cells


def solution(mesh):
    return jax.shard_map(
        per_device,
        mesh=mesh,
        in_specs=(
            P(("group", "dom"), None),
            P(("group", "dom"), None),
            P(("group", "dom"), None),
            P(),
            P(("group", "dom"), None, None, None),
            P(("group", "dom"), None),
            P(("group", "dom")),
            P(("group", "dom"), None, None),
        ),
        out_specs=(P(None, ("group", "dom"), None), P()),
        check_vma=False,
    )
```

```python
import functools
import jax
import jax.numpy as jnp
from jax import lax
from jax.experimental import pallas as pl
from jax.experimental.pallas import tpu as pltpu
from jax.sharding import PartitionSpec as P

def table_kernel(cols, live, need, tbl, *, rows, nslots, halo):
    far = 10 * rows

    def build(b, carry):
        n = live[b]
        for s in range(nslots):
            c = cols[b, s]
            local = c < rows
            q = jnp.maximum(c - rows, 0)
            k = q // halo
            row = jnp.where(local, c, 2 * rows * (k + 1) + need[k, q % halo])
            tbl[b * nslots + s] = jnp.where(s < n, row, far)
        return carry

    lax.fori_loop(0, rows, build, 0)


def step_kernel(tbl, shifts, cur, diag, h0, h1, h2, h3, a_ref, out, ext, halves, *, step, rows, nslots):
    bs = ext.shape[1]
    half = bs // 2
    far = 10 * rows
    for k, h in enumerate((cur, h0, h1, h2, h3)):
        ext[2 * rows * k : 2 * rows * (k + 1), :] = h[...]
    ext[far:, :] = jnp.zeros((ext.shape[0] - far, bs), jnp.float32)
    halves[...] = jnp.zeros(halves.shape, halves.dtype)
    low = lax.broadcasted_iota(jnp.int32, (bs, bs), 1) < half
    r = lax.broadcasted_iota(jnp.int32, (8, 2 * bs), 0)
    c = lax.broadcasted_iota(jnp.int32, (8, 2 * bs), 1) % bs
    pick = (((r == 0) & (c < half)) | ((r == 1) & (c >= half))).astype(jnp.float32).astype(jnp.bfloat16)

    def lane_sums(at):
        sums = lax.dot_general(
            pick, halves[...], (((1,), (1,)), ((), ())), preferred_element_type=jnp.float32
        )
        for u in range(2):
            out[pl.ds(at + u, 1), :] = sums[0:1, u * bs : (u + 1) * bs]
            out[pl.ds(rows + at + u, 1), :] = sums[1:2, u * bs : (u + 1) * bs]

    def pair(g, carry):
        lane_sums(jnp.maximum(2 * g - 2, 0))
        for u in range(2):
            first = (2 * g + u) * nslots
            ap = ar = None
            for s in range(nslots):
                at = tbl[first + s]
                a = a_ref[first + s]
                tp = a * ext[pl.ds(at, 1), :]
                tr = a * ext[pl.ds(at + rows, 1), :]
                ap = tp if ap is None else ap + tp
                ar = tr if ar is None else ar + tr
            both = jnp.where(low, ap + pltpu.roll(ap, half, 1), ar + pltpu.roll(ar, half, 1))
            hi = both.astype(jnp.bfloat16)
            lo = (both - hi.astype(jnp.float32)).astype(jnp.bfloat16)
            halves[u * bs : (u + 1) * bs, 0:bs] = hi
            halves[u * bs : (u + 1) * bs, bs:] = lo
        return carry

    lax.fori_loop(0, rows // 2, pair, 0)
    lane_sums(rows - 2)
    d = diag[...] - shifts[step]
    out[0:rows, :] += d * cur[0:rows, :]
    out[rows : 2 * rows, :] += d * cur[rows : 2 * rows, :]


def sum_over(x, axis):
    n = lax.axis_size(axis)
    if n & (n - 1):
        return lax.psum(x, axis)
    d = 1
    while d < n:
        x = x + lax.ppermute(x, axis, [(i, i ^ d) for i in range(n)])
        d *= 2
    return x


def per_device(p_start, r_start, diag_shift, shifts, block_values, block_cols, live_slots, needed):
    rows, bs = p_start.shape
    nslots = block_values.shape[1]
    halo = needed.shape[2]
    depth = shifts.shape[0]
    f32 = jnp.float32
    smem = pl.BlockSpec(memory_space=pltpu.SMEM)
    vmem = pl.BlockSpec(memory_space=pltpu.VMEM)
    field = jax.ShapeDtypeStruct((2 * rows, bs), f32)
    scratch = [pltpu.VMEM((10 * rows + rows + 8, bs), f32), pltpu.VMEM((2 * bs, 2 * bs), jnp.bfloat16)]
    params = pltpu.CompilerParams(vmem_limit_bytes=24 * 1024 * 1024)
    a_flat = block_values.reshape(rows * nslots, bs, bs)
    tbl = pl.pallas_call(
        functools.partial(table_kernel, rows=rows, nslots=nslots, halo=halo),
        out_shape=jax.ShapeDtypeStruct((rows * nslots,), jnp.int32),
        in_specs=[smem, smem, smem],
        out_specs=smem,
        name="table",
    )(block_cols, live_slots, needed[0])

    def halos(cur):
        nd, ng = lax.axis_size("dom"), lax.axis_size("group")
        up = [(i, (i + 1) % nd) for i in range(nd)]
        down = [((i + 1) % nd, i) for i in range(nd)]
        gup = [(i, (i + 1) % ng) for i in range(ng)]
        gdown = [((i + 1) % ng, i) for i in range(ng)]
        return (
            lax.ppermute(cur, "dom", up),
            lax.ppermute(cur, "dom", down),
            lax.ppermute(cur, "group", gup),
            lax.ppermute(cur, "group", gdown),
        )

    cur = jnp.concatenate([p_start, r_start], axis=0)
    fields = [cur]
    for step in range(depth):
        h = halos(cur)
        cur = pl.pallas_call(
            functools.partial(step_kernel, step=step, rows=rows, nslots=nslots),
            out_shape=field,
            in_specs=[smem, smem] + [vmem] * 7,
            out_specs=vmem,
            scratch_shapes=scratch,
            compiler_params=params,
            name="step",
        )(tbl, shifts, cur, diag_shift, *h, a_flat)
        fields.append(cur)
    both = jnp.stack(fields).reshape(depth + 1, 2, rows, bs)
    basis = jnp.concatenate([both[:, 0], both[:depth, 1]], axis=0)
    total_cells = rows * bs * lax.axis_size("group") * lax.axis_size("dom")
    local_gram = jnp.einsum("kbi,lbi->kl", basis, basis, precision=lax.Precision.HIGHEST)
    return basis, sum_over(sum_over(local_gram, "dom"), "group") / total_cells


def solution(mesh):
    return jax.shard_map(
        per_device,
        mesh=mesh,
        in_specs=(
            P(("group", "dom"), None),
            P(("group", "dom"), None),
            P(("group", "dom"), None),
            P(),
            P(("group", "dom"), None, None, None),
            P(("group", "dom"), None),
            P(("group", "dom")),
            P(("group", "dom"), None, None),
        ),
        out_specs=(P(None, ("group", "dom"), None), P()),
        check_vma=False,
    )
```

```python
import functools
import jax
import jax.numpy as jnp
from jax import lax
from jax.experimental import pallas as pl
from jax.experimental.pallas import tpu as pltpu
from jax.sharding import PartitionSpec as P

def build_table(cols, live, need, tbl, rows, nslots, halo):
    far = 10 * rows

    def build(b, carry):
        n = live[b]
        for s in range(nslots):
            c = cols[b, s]
            local = c < rows
            q = jnp.maximum(c - rows, 0)
            k = q // halo
            row = jnp.where(local, c, 2 * rows * (k + 1) + need[k, q % halo])
            tbl[b * nslots + s] = jnp.where(s < n, row, far)
        return carry

    lax.fori_loop(0, rows, build, 0)


def first_kernel(cols, live, need, shifts, cur, diag, h0, h1, h2, h3, a_hbm, out, a_vmem, tbl, ext, halves, sems, *, rows, nslots, halo):
    def copy(g):
        at = pl.ds(g * 2 * nslots, 2 * nslots)
        return pltpu.make_async_copy(a_hbm.at[at], a_vmem.at[at], sems.at[g])

    def start(g, carry):
        copy(g).start()
        return carry

    lax.fori_loop(0, rows // 2, start, 0)
    build_table(cols, live, need, tbl, rows, nslots, halo)
    step_kernel(
        tbl, shifts, cur, diag, h0, h1, h2, h3, a_vmem, out, ext, halves,
        step=0, last=False, rows=rows, nslots=nslots, ready=lambda g: copy(g).wait(),
    )


def step_kernel(
    tbl, shifts, cur, diag, h0, h1, h2, h3, a_ref, out, ext, halves, *, step, last, rows, nslots, ready=None
):
    bs = ext.shape[1]
    half = bs // 2
    far = 10 * rows
    for k, h in enumerate((cur, h0, h1, h2, h3)):
        ext[2 * rows * k : 2 * rows * (k + 1), :] = h[...]
    ext[far:, :] = jnp.zeros((ext.shape[0] - far, bs), jnp.float32)
    halves[...] = jnp.zeros(halves.shape, halves.dtype)
    low = lax.broadcasted_iota(jnp.int32, (bs, bs), 1) < half
    r = lax.broadcasted_iota(jnp.int32, (8, 2 * bs), 0)
    c = lax.broadcasted_iota(jnp.int32, (8, 2 * bs), 1) % bs
    pick = (((r == 0) & (c < half)) | ((r == 1) & (c >= half))).astype(jnp.float32).astype(jnp.bfloat16)

    def lane_sums(at):
        sums = lax.dot_general(
            pick, halves[...], (((1,), (1,)), ((), ())), preferred_element_type=jnp.float32
        )
        for u in range(2):
            out[pl.ds(at + u, 1), :] = sums[0:1, u * bs : (u + 1) * bs]
            out[pl.ds(rows + at + u, 1), :] = sums[1:2, u * bs : (u + 1) * bs]

    def pair(g, carry):
        if ready is not None:
            ready(g)
        lane_sums(jnp.maximum(2 * g - 2, 0))
        for u in range(2):
            first = (2 * g + u) * nslots
            ap = ar = None
            for s in range(nslots):
                at = tbl[first + s]
                a = a_ref[first + s]
                tp = a * ext[pl.ds(at, 1), :]
                ap = tp if ap is None else ap + tp
                if not last:
                    tr = a * ext[pl.ds(at + rows, 1), :]
                    ar = tr if ar is None else ar + tr
            both = ap + pltpu.roll(ap, half, 1)
            if not last:
                both = jnp.where(low, both, ar + pltpu.roll(ar, half, 1))
            hi = both.astype(jnp.bfloat16)
            lo = (both - hi.astype(jnp.float32)).astype(jnp.bfloat16)
            halves[u * bs : (u + 1) * bs, 0:bs] = hi
            halves[u * bs : (u + 1) * bs, bs:] = lo
        return carry

    lax.fori_loop(0, rows // 2, pair, 0)
    lane_sums(rows - 2)
    d = diag[...] - shifts[step]
    out[0:rows, :] += d * cur[0:rows, :]
    out[rows : 2 * rows, :] += d * cur[rows : 2 * rows, :]


def sum_over(x, axis):
    n = lax.axis_size(axis)
    if n & (n - 1):
        return lax.psum(x, axis)
    d = 1
    while d < n:
        wide = min(8, n // d)
        parts = [lax.ppermute(x, axis, [(i, i ^ (d * k)) for i in range(n)]) for k in range(1, wide)]
        parts = [x] + parts
        while len(parts) > 1:
            parts = [parts[k] + parts[k + 1] for k in range(0, len(parts), 2)]
        x = parts[0]
        d *= wide
    return x


def per_device(p_start, r_start, diag_shift, shifts, block_values, block_cols, live_slots, needed):
    rows, bs = p_start.shape
    nslots = block_values.shape[1]
    halo = needed.shape[2]
    depth = shifts.shape[0]
    f32 = jnp.float32
    smem = pl.BlockSpec(memory_space=pltpu.SMEM)
    vmem = pl.BlockSpec(memory_space=pltpu.VMEM)
    field = jax.ShapeDtypeStruct((2 * rows, bs), f32)
    scratch = [pltpu.VMEM((10 * rows + rows + 8, bs), f32), pltpu.VMEM((2 * bs, 2 * bs), jnp.bfloat16)]
    params = pltpu.CompilerParams(vmem_limit_bytes=4 * 1024 * 1024)
    a_flat = pltpu.with_memory_space_constraint(block_values.reshape(rows * nslots, bs, bs), pltpu.HBM)
    def halos(cur):
        nd, ng = lax.axis_size("dom"), lax.axis_size("group")
        up = [(i, (i + 1) % nd) for i in range(nd)]
        down = [((i + 1) % nd, i) for i in range(nd)]
        gup = [(i, (i + 1) % ng) for i in range(ng)]
        gdown = [((i + 1) % ng, i) for i in range(ng)]
        return (
            lax.ppermute(cur, "dom", up),
            lax.ppermute(cur, "dom", down),
            lax.ppermute(cur, "group", gup),
            lax.ppermute(cur, "group", gdown),
        )

    cur = jnp.concatenate([p_start, r_start], axis=0)
    fields = [cur]
    for step in range(depth):
        h = halos(cur)
        if step == 0:
            cur, a_vmem, tbl = pl.pallas_call(
                functools.partial(first_kernel, rows=rows, nslots=nslots, halo=halo),
                out_shape=(
                    field,
                    pltpu.VMEM((rows * nslots, bs, bs), f32),
                    jax.ShapeDtypeStruct((rows * nslots,), jnp.int32),
                ),
                in_specs=[smem] * 4 + [vmem] * 6 + [pl.BlockSpec(memory_space=pltpu.HBM)],
                out_specs=(vmem, vmem, smem),
                scratch_shapes=scratch + [pltpu.SemaphoreType.DMA((rows // 2,))],
                compiler_params=params,
                name="first",
            )(block_cols, live_slots, needed[0], shifts, cur, diag_shift, *h, a_flat)
        else:
            cur = pl.pallas_call(
                functools.partial(step_kernel, step=step, last=step == depth - 1, rows=rows, nslots=nslots),
                out_shape=field,
                in_specs=[smem, smem] + [vmem] * 7,
                out_specs=vmem,
                scratch_shapes=scratch,
                compiler_params=params,
                name="step",
            )(tbl, shifts, cur, diag_shift, *h, a_vmem)
        fields.append(cur)
    both = jnp.stack(fields).reshape(depth + 1, 2, rows, bs)
    basis = jnp.concatenate([both[:, 0], both[:depth, 1]], axis=0)
    total_cells = rows * bs * lax.axis_size("group") * lax.axis_size("dom")
    local_gram = jnp.einsum("kbi,lbi->kl", basis, basis, precision=lax.Precision.HIGHEST)
    return basis, sum_over(sum_over(local_gram, "dom"), "group") / total_cells


def solution(mesh):
    return jax.shard_map(
        per_device,
        mesh=mesh,
        in_specs=(
            P(("group", "dom"), None),
            P(("group", "dom"), None),
            P(("group", "dom"), None),
            P(),
            P(("group", "dom"), None, None, None),
            P(("group", "dom"), None),
            P(("group", "dom")),
            P(("group", "dom"), None, None),
        ),
        out_specs=(P(None, ("group", "dom"), None), P()),
        check_vma=False,
    )
```

```python
import functools
import jax
import jax.numpy as jnp
from jax import lax
from jax.experimental import pallas as pl
from jax.experimental.pallas import tpu as pltpu
from jax.sharding import PartitionSpec as P

def build_table(cols, live, need, tbl, rows, nslots, halo):
    far = 10 * rows

    def build(b, carry):
        n = live[b]
        for s in range(nslots):
            c = cols[b, s]
            local = c < rows
            q = jnp.maximum(c - rows, 0)
            k = q // halo
            row = jnp.where(local, c, 2 * rows * (k + 1) + need[k, q % halo])
            tbl[b * nslots + s] = jnp.where(s < n, row, far)
        return carry

    lax.fori_loop(0, rows, build, 0)


def first_kernel(cols, live, need, shifts, cur, diag, h0, h1, h2, h3, a_hbm, out, a_vmem, tbl, ext, halves, sems, *, rows, nslots, halo):
    def copy(g):
        at = pl.ds(g * 2 * nslots, 2 * nslots)
        return pltpu.make_async_copy(a_hbm.at[at], a_vmem.at[at], sems.at[g])

    def start(g, carry):
        copy(g).start()
        return carry

    lax.fori_loop(0, rows // 2, start, 0)
    build_table(cols, live, need, tbl, rows, nslots, halo)
    step_kernel(
        tbl, shifts, cur, diag, h0, h1, h2, h3, a_vmem, out, ext, halves,
        step=0, last=False, rows=rows, nslots=nslots, ready=lambda g: copy(g).wait(),
    )


def step_kernel(
    tbl, shifts, cur, diag, h0, h1, h2, h3, a_ref, out, ext, halves, *, step, last, rows, nslots, ready=None
):
    bs = ext.shape[1]
    half = bs // 2
    far = 10 * rows
    for k, h in enumerate((cur, h0, h1, h2, h3)):
        ext[2 * rows * k : 2 * rows * (k + 1), :] = h[...]
    ext[far:, :] = jnp.zeros((ext.shape[0] - far, bs), jnp.float32)
    halves[...] = jnp.zeros(halves.shape, halves.dtype)
    low = lax.broadcasted_iota(jnp.int32, (bs, bs), 1) < half
    r = lax.broadcasted_iota(jnp.int32, (8, 2 * bs), 0)
    c = lax.broadcasted_iota(jnp.int32, (8, 2 * bs), 1) % bs
    pick = (((r == 0) & (c < half)) | ((r == 1) & (c >= half))).astype(jnp.float32).astype(jnp.bfloat16)

    def lane_sums(at):
        sums = lax.dot_general(
            pick, halves[...], (((1,), (1,)), ((), ())), preferred_element_type=jnp.float32
        )
        for u in range(2):
            out[pl.ds(at + u, 1), :] = sums[0:1, u * bs : (u + 1) * bs]
            out[pl.ds(rows + at + u, 1), :] = sums[1:2, u * bs : (u + 1) * bs]

    def pair(g, carry):
        if ready is not None:
            ready(g)
        lane_sums(jnp.maximum(2 * g - 2, 0))
        for u in range(2):
            first = (2 * g + u) * nslots
            ap = ar = None
            for s in range(nslots):
                at = tbl[first + s]
                a = a_ref[first + s]
                tp = a * ext[pl.ds(at, 1), :]
                ap = tp if ap is None else ap + tp
                if not last:
                    tr = a * ext[pl.ds(at + rows, 1), :]
                    ar = tr if ar is None else ar + tr
            both = ap + pltpu.roll(ap, half, 1)
            if not last:
                both = jnp.where(low, both, ar + pltpu.roll(ar, half, 1))
            hi = both.astype(jnp.bfloat16)
            lo = (both - hi.astype(jnp.float32)).astype(jnp.bfloat16)
            halves[u * bs : (u + 1) * bs, 0:bs] = hi
            halves[u * bs : (u + 1) * bs, bs:] = lo
        return carry

    lax.fori_loop(0, rows // 2, pair, 0)
    lane_sums(rows - 2)
    d = diag[...] - shifts[step]
    out[0:rows, :] += d * cur[0:rows, :]
    out[rows : 2 * rows, :] += d * cur[rows : 2 * rows, :]


def sum_over(x, axis):
    n = lax.axis_size(axis)
    if n & (n - 1):
        return lax.psum(x, axis)
    d = 1
    while d < n:
        wide = min(8, n // d)
        parts = [lax.ppermute(x, axis, [(i, i ^ (d * k)) for i in range(n)]) for k in range(1, wide)]
        parts = [x] + parts
        while len(parts) > 1:
            parts = [parts[k] + parts[k + 1] for k in range(0, len(parts), 2)]
        x = parts[0]
        d *= wide
    return x


def per_device(p_start, r_start, diag_shift, shifts, block_values, block_cols, live_slots, needed):
    rows, bs = p_start.shape
    nslots = block_values.shape[1]
    halo = needed.shape[2]
    depth = shifts.shape[0]
    f32 = jnp.float32
    smem = pl.BlockSpec(memory_space=pltpu.SMEM)
    vmem = pl.BlockSpec(memory_space=pltpu.VMEM)
    field = jax.ShapeDtypeStruct((2 * rows, bs), f32)
    scratch = [pltpu.VMEM((10 * rows + rows + 8, bs), f32), pltpu.VMEM((2 * bs, 2 * bs), jnp.bfloat16)]
    params = pltpu.CompilerParams(vmem_limit_bytes=4 * 1024 * 1024)
    a_flat = pltpu.with_memory_space_constraint(block_values.reshape(rows * nslots, bs, bs), pltpu.HBM)
    def halos(cur):
        nd, ng = lax.axis_size("dom"), lax.axis_size("group")
        up = [(i, (i + 1) % nd) for i in range(nd)]
        down = [((i + 1) % nd, i) for i in range(nd)]
        gup = [(i, (i + 1) % ng) for i in range(ng)]
        gdown = [((i + 1) % ng, i) for i in range(ng)]
        return (
            lax.ppermute(cur, "dom", up),
            lax.ppermute(cur, "dom", down),
            lax.ppermute(cur, "group", gup),
            lax.ppermute(cur, "group", gdown),
        )

    cur = jnp.concatenate([p_start, r_start], axis=0)
    fields = [cur]
    for step in range(depth):
        h = halos(cur)
        if step == 0:
            cur, a_vmem, tbl = pl.pallas_call(
                functools.partial(first_kernel, rows=rows, nslots=nslots, halo=halo),
                out_shape=(
                    field,
                    pltpu.VMEM((rows * nslots, bs, bs), f32),
                    jax.ShapeDtypeStruct((rows * nslots,), jnp.int32),
                ),
                in_specs=[smem] * 4 + [vmem] * 6 + [pl.BlockSpec(memory_space=pltpu.HBM)],
                out_specs=(vmem, vmem, smem),
                scratch_shapes=scratch + [pltpu.SemaphoreType.DMA((rows // 2,))],
                compiler_params=params,
                name="first",
            )(block_cols, live_slots, needed[0], shifts, cur, diag_shift, *h, a_flat)
        else:
            cur = pl.pallas_call(
                functools.partial(step_kernel, step=step, last=step == depth - 1, rows=rows, nslots=nslots),
                out_shape=field,
                in_specs=[smem, smem] + [vmem] * 7,
                out_specs=vmem,
                scratch_shapes=scratch,
                compiler_params=params,
                name="step",
            )(tbl, shifts, cur, diag_shift, *h, a_vmem)
        fields.append(cur)
    fields = lax.optimization_barrier(fields)
    both = jnp.stack(fields).reshape(depth + 1, 2, rows, bs)
    basis = jnp.concatenate([both[:, 0], both[:depth, 1]], axis=0)
    total_cells = rows * bs * lax.axis_size("group") * lax.axis_size("dom")
    local_gram = jnp.einsum("kbi,lbi->kl", basis, basis, precision=lax.Precision.HIGHEST)
    return basis, sum_over(sum_over(local_gram, "dom"), "group") / total_cells


def solution(mesh):
    return jax.shard_map(
        per_device,
        mesh=mesh,
        in_specs=(
            P(("group", "dom"), None),
            P(("group", "dom"), None),
            P(("group", "dom"), None),
            P(),
            P(("group", "dom"), None, None, None),
            P(("group", "dom"), None),
            P(("group", "dom")),
            P(("group", "dom"), None, None),
        ),
        out_specs=(P(None, ("group", "dom"), None), P()),
        check_vma=False,
    )
```
